256 devices in a mesh: groups: 2 (over z), ep: 16 (over x, core), tp: 8 (over y).
Axes of the slice: x: 8, y: 8, z: 2, core: 2. Of those that a mesh axis runs over, the one named last changes fastest.
The devices are a block of a 8x8x16 slice.
Arguments:
- tokens: bfloat16 [1024, 7168], P(('groups', 'ep')), parts along dimension 0, may hold values from -6 to 6
- w_gate: bfloat16 [16, 7168, 2048], P('ep', None, 'tp'), may hold values from -0.0625 to 0.0625
- w_up: bfloat16 [16, 7168, 2048], P('ep', None, 'tp'), may hold values from -0.0625 to 0.0625
- w_down: bfloat16 [16, 2048, 7168], P('ep', 'tp'), may hold values from -0.1875 to 0.1875
- router_logits: float32 [1024, 8], P(('groups', 'ep')), parts along dimension 0, may hold values from -6 to 6
- expert_ids: int32 [1024, 8], P(('groups', 'ep')), parts along dimension 0, may hold values from 0 to 15, all different within a row; in each aligned block of 32 rows (0 to 31, 32 to 63, ...) at most 24 rows name the same one
- draft_lengths: int32 [128], P(('groups', 'ep')), parts along dimension 0, may hold values from 7 to 8
- accept_mask: int32 [128, 8], P(('groups', 'ep')), parts along dimension 0, may hold values 0 or 1
Outputs:
- mixed: bfloat16 [1024, 7168], P(('groups', 'ep'), 'tp'), parts along dimension 0
- accepted: int32 [2], P('groups'), parts along dimension 0
The draws below stay inside these ranges and needn't reach their ends.
There are 2 independent parts, one for each index of `groups`. The reference program is written for one: setup_inputs(seed, part) draws one part's arguments, and reference() takes and returns one part's arrays. A program takes and returns all parts, laid end to end along the dimension named above; an argument that names none is the same for every part. Nothing has to cross between parts.
Inputs may be any that keep to these rules, and one draw needn't show every extreme that they name: `expert_ids`: each row names 8 different experts. Among the rows of one ep index (aligned blocks of 32 rows) no expert is named by more than 24 rows, and in every draw some expert is named by exactly 24 rows of some block.
All inputs are finite; a program needn't handle non-finite values. No bound on the sum of `accept_mask` on one device may be relied on, other than what follows from the above.
Results may differ from the reference program's by a relative error of at most 0.017.
Values may be sent and summed in bfloat16 or wider, within the bound.
No kernel may reach another device: no remote copies, remote signals or barrier semaphores. Data moves between devices by JAX's collectives and lax.ppermute only.
A program may use at most 128 MiB of HBM per device.

```python
import math
import jax
import jax.numpy as jnp
import numpy as np
from jax import lax

D = 7168
FF = 2048
TOP = 8
DRAFT = 8
EXPERTS = 16
TOK_DEV = 32
REQUESTS = 64
TOKENS = 512
CAP = 24
N_EP = 16
N_TP = 8


def set_ends(result, own_key, smallest, high):
    shape = result.shape
    spot = [jax.random.randint(jax.random.fold_in(own_key, axis), (), 0, shape[axis]) for axis in range(len(shape))]
    result = result.at[tuple(spot)].set(smallest)
    longest = shape.index(max(shape))
    spot[longest] = (spot[longest] + 1) % shape[longest]
    return result.at[tuple(spot)].set(high)


def raised(entries, rng, source, target, blocks, factor):
    owner, partner = [(jnp.arange(entries.shape[position]) // (entries.shape[position] // blocks)).reshape([-1 if axis == position else 1 for axis in range(entries.ndim)]) for position in (source, target)]
    chosen = jax.random.permutation(rng, blocks)[partner]
    strong = (owner == chosen) | (owner == (partner + blocks // 2) % blocks)
    return jnp.where(strong, factor * entries, entries)


def block_levels(own_key, extent, shards, low, high):
    gain, own = 1.0, jax.random.fold_in(own_key, 6)
    for axis_at, blocks in shards:
        draws = jnp.exp(jax.random.uniform(jax.random.fold_in(own, axis_at), (blocks,), jnp.float32, low / len(shards), high / len(shards)))
        gain = gain * jnp.repeat(draws, extent[axis_at] // blocks).reshape([-1 if axis == axis_at else 1 for axis in range(len(extent))])
    return gain


def shared_out(own_key, own, number, rows, count, top, reach, lean):
    order = jax.random.permutation(own_key, count)
    heavy_load, common = shares(count, rows * top, reach, lean, True), shares(count, rows * top, reach, lean, False)
    places = jnp.arange(count)

    def named(tallies, rotation):
        used = int((tallies > 0).sum())
        fixed = max(1, used // 4)
        shifted = fixed + (places - fixed + rotation * (used - fixed)) % max(1, count - fixed)
        return jnp.zeros((count,), jnp.int32).at[order[jnp.where(places < fixed, places, shifted)]].set(jnp.asarray(tallies, jnp.int32))

    tallies = jnp.where(number % 4 == 0, named(heavy_load, number // 4), named(common, number - number // 4 - 1))
    mixed = jax.random.permutation(jax.random.fold_in(own, 3), count)
    giver, taker = mixed[0:count // 2 * 2:2], mixed[1:count // 2 * 2:2]
    slack = jnp.minimum(tallies[giver] - 1, reach - tallies[taker]) // 2
    slack = jnp.where((giver == order[0]) | (taker == order[0]) | (tallies[taker] == 0), 0, jnp.maximum(slack, 0))
    shifted = jax.random.randint(jax.random.fold_in(own, 4), (count // 2,), 0, 1 << 20) % (slack + 1)
    tallies = tallies.at[giver].add(-shifted).at[taker].add(shifted)
    labels = jnp.searchsorted(jnp.cumsum(tallies), jnp.arange(rows * top), side="right").astype(jnp.int32)
    listing = labels.reshape(top, rows).T
    listing = listing[jax.random.permutation(jax.random.fold_in(own, 1), rows)]
    rotation = jax.random.randint(jax.random.fold_in(own, 2), (rows, 1), 0, top)
    return jnp.take_along_axis(listing, (jnp.arange(top)[None, :] + rotation) % top, axis=1)


def shares(amount, total, limit, skew, full):
    loads = [(1 << 20) // math.isqrt(rank ** skew) + 1 for rank in range(1, amount + 1)]
    largest = limit if full else min(limit, max(-(-total // amount), total * loads[0] // sum(loads)))
    least = 1 if total - largest >= amount - 1 else 0
    given, surplus = [largest] + [least] * (amount - 1), total - largest - least * (amount - 1)
    while surplus > 0:
        movable = [i for i in range(1, amount) if given[i] < largest] or [i for i in range(1, amount) if given[i] < limit]
        whole, remaining = sum([loads[i] for i in movable]), surplus
        for i in movable:
            extra = min(limit - given[i], max(1, remaining * loads[i] // whole), surplus)
            given[i] = given[i] + extra
            surplus = surplus - extra
    return np.array(given)


def bell_draw(stream_key, shape, scale, bound, shards=(), held_as=jnp.bfloat16):
    values = jax.random.normal(stream_key, shape, jnp.float32) * scale
    if len(shards) > 0:
        values = block_levels(stream_key, shape, shards, -0.22, 0.18) * values
    return jnp.clip(values, min=-bound, max=bound).astype(held_as)


def gaussian_with(rng, shape, deviation, bound, shards, heavy, kind=jnp.bfloat16):
    drawn = deviation * jax.random.normal(rng, shape, jnp.float32)
    if shards:
        drawn = drawn * block_levels(rng, shape, shards, -0.22, 0.18)
    return jnp.clip(raised(drawn, jax.random.fold_in(rng, 3), *heavy), -bound, bound).astype(kind)


def setup_inputs(seed: int = 0, part: int = 0) -> dict:
    arg_keys = jax.random.split(jax.random.key(seed), 9)
    own_keys = jax.random.split(jax.random.fold_in(arg_keys[8], part), 9)
    tokens = bell_draw(own_keys[0], (TOKENS, D), 1.0, 6.0, ((0, 16),))
    w_gate = bell_draw(arg_keys[1], (EXPERTS, D, FF), D ** -0.5, 0.0625, ((0, 16), (2, 8)))
    w_up = bell_draw(arg_keys[2], (EXPERTS, D, FF), D ** -0.5, 0.0625, ((0, 16), (2, 8)))
    w_down = gaussian_with(arg_keys[3], (EXPERTS, FF, D), FF ** -0.5, 0.1875, ((0, 16), (1, 8)), (1, 2, 8, 2.0))
    router_logits = bell_draw(own_keys[4], (TOKENS, TOP), 1.5, 6.0, ((0, 16),), jnp.float32)
    expert_ids_keys = jax.random.split(jax.random.fold_in(own_keys[5], 1), TOKENS // TOK_DEV)
    expert_ids_turns = jax.random.permutation(jax.random.fold_in(own_keys[5], 3), TOKENS // TOK_DEV)
    expert_ids = jax.vmap(lambda own, number: shared_out(jax.random.fold_in(own_keys[5], 2), own, number, TOK_DEV, EXPERTS, TOP, CAP, 2))(expert_ids_keys, expert_ids_turns).reshape((TOKENS, TOP))
    draft_lengths = set_ends(jax.random.randint(own_keys[6], (REQUESTS,), DRAFT - 1, DRAFT + 1), jax.random.fold_in(own_keys[6], 1), DRAFT - 1, DRAFT).astype(jnp.int32)
    accept_mask = set_ends((jax.random.randint(own_keys[7], (REQUESTS, DRAFT), 0, 4) < 3).astype(jnp.int32), jax.random.fold_in(own_keys[7], 1), 0, 1)
    return dict(tokens=tokens, w_gate=w_gate, w_up=w_up, w_down=w_down, router_logits=router_logits, expert_ids=expert_ids, draft_lengths=draft_lengths, accept_mask=accept_mask)


def reference(tokens, w_gate, w_up, w_down, router_logits, expert_ids, draft_lengths, accept_mask):
    live = jnp.arange(DRAFT, dtype=jnp.int32)[None, :] < draft_lengths[:, None]
    live_rows = live.reshape(TOKENS)
    live_tokens = jnp.where(live_rows[:, None], tokens, jnp.zeros((), tokens.dtype))
    sig = jax.nn.sigmoid(router_logits.astype(jnp.float32))
    gates = 2.827 * sig / jnp.sum(sig, axis=1, keepdims=True)
    load = N_EP * CAP
    flat_ids = expert_ids.reshape(-1).astype(jnp.int32)
    onehot = (flat_ids[:, None] == jnp.arange(EXPERTS, dtype=jnp.int32)[None, :]).astype(jnp.int32)
    rank = jnp.cumsum(onehot, axis=0) - 1
    slot = jnp.sum(rank * onehot, axis=1).astype(jnp.int32)
    source = (jnp.arange(TOKENS * TOP, dtype=jnp.int32) // TOP).astype(jnp.int32)
    table = jnp.zeros((EXPERTS, load), jnp.int32).at[flat_ids, slot].set(source)
    filled = jnp.zeros((EXPERTS, load), jnp.int32).at[flat_ids, slot].set(1)

    def one_expert(items):
        weight_g, weight_u, weight_d, rows_of, used = items
        rows = jnp.where(used[:, None] > 0, live_tokens[rows_of], jnp.zeros((), tokens.dtype))
        gate = jnp.dot(rows, weight_g, preferred_element_type=jnp.float32)
        up = jnp.dot(rows, weight_u, preferred_element_type=jnp.float32)
        hidden = (jax.nn.silu(gate) * up).astype(jnp.bfloat16)
        blocks = hidden.reshape(load, N_TP, FF // N_TP).astype(jnp.float32)
        down = weight_d.reshape(N_TP, FF // N_TP, D).astype(jnp.float32)
        parts = jnp.einsum('mtf,tfd->tmd', blocks, down)
        summed = jnp.sum(parts.astype(jnp.bfloat16).astype(jnp.float32), axis=0)
        return summed.astype(jnp.bfloat16)

    outs = lax.map(one_expert, (w_gate, w_up, w_down, table, filled))
    picked = outs[flat_ids, slot].reshape(TOKENS, TOP, D).astype(jnp.float32)
    mixed = jnp.sum(gates[:, :, None] * picked, axis=1).astype(jnp.bfloat16)
    passed = accept_mask.astype(jnp.int32) * live.astype(jnp.int32)
    prefix = jnp.cumprod(passed, axis=1)
    accepted = jnp.sum(prefix).astype(jnp.int32).reshape(1)
    return mixed, accepted
```

```python
import functools
import jax
import jax.numpy as jnp
from jax import lax
from jax.experimental import pallas as pl
from jax.experimental.pallas import tpu as pltpu
from jax.sharding import PartitionSpec as P

DRAFT = 8


def ffn_kernel(n, x_ref, wg_ref, wu_ref, wd_ref, gate_ref, o_ref, acc_g, acc_u, hid):
    step = pl.program_id(0)

    @pl.when(step == 0)
    def _():
        acc_g[...] = jnp.zeros_like(acc_g)
        acc_u[...] = jnp.zeros_like(acc_u)

    @pl.when(step < n)
    def _():
        x = x_ref[...].reshape(acc_g.shape[0], x_ref.shape[3])
        acc_g[...] += jnp.dot(x, wg_ref[0], preferred_element_type=jnp.float32)
        acc_u[...] += jnp.dot(x, wu_ref[0], preferred_element_type=jnp.float32)

    @pl.when(step == n - 1)
    def _():
        g = acc_g[...]
        hid[...] = (g / (1.0 + jnp.exp(-g)) * acc_u[...]).astype(jnp.bfloat16)

    @pl.when(step >= n)
    def _():
        p = jnp.dot(hid[...], wd_ref[0], preferred_element_type=jnp.float32)
        p = p * gate_ref[...]
        o_ref[...] = p.astype(jnp.bfloat16).reshape(o_ref.shape)


def expert(gathered, w_gate, w_up, w_down, gate):
    ep, n, rows, width = gathered.shape
    units = w_gate.shape[2]
    total = ep * rows
    return pl.pallas_call(
        functools.partial(ffn_kernel, n),
        grid=(2 * n,),
        in_specs=[
            pl.BlockSpec((ep, 1, rows, width), lambda s: (0, jnp.minimum(s, n - 1), 0, 0)),
            pl.BlockSpec((1, width, units), lambda s: (0, jnp.minimum(s, n - 1), 0)),
            pl.BlockSpec((1, width, units), lambda s: (0, jnp.minimum(s, n - 1), 0)),
            pl.BlockSpec((1, units, width), lambda s: (0, 0, jnp.maximum(s - n, 0))),
            pl.BlockSpec((total, 1), lambda s: (0, 0)),
        ],
        out_specs=pl.BlockSpec((ep, 1, rows, width), lambda s: (0, jnp.maximum(s - n, 0), 0, 0)),
        out_shape=jax.ShapeDtypeStruct(gathered.shape, jnp.bfloat16),
        scratch_shapes=[
            pltpu.VMEM((total, units), jnp.float32),
            pltpu.VMEM((total, units), jnp.float32),
            pltpu.VMEM((total, units), jnp.bfloat16),
        ],
        cost_estimate=pl.CostEstimate(
            flops=6 * total * n * width * units,
            bytes_accessed=4 * total * n * width + 6 * n * width * units,
            transcendentals=total * units,
        ),
        compiler_params=pltpu.CompilerParams(dimension_semantics=("arbitrary",)),
    )(gathered, w_gate, w_up, w_down, gate)


def per_device(tokens, w_gate, w_up, w_down, router_logits, expert_ids, draft_lengths, accept_mask):
    rows, width = tokens.shape
    ep = lax.axis_size("ep")
    tp = lax.axis_size("tp")
    slice_width = width // tp
    live = jnp.arange(DRAFT, dtype=jnp.int32)[None, :] < draft_lengths[:, None]
    live_rows = live.reshape(rows)
    own_cols = lax.dynamic_slice_in_dim(tokens, lax.axis_index("tp") * slice_width, slice_width, 1)
    own_cols = jnp.where(live_rows[:, None], own_cols, jnp.zeros((), tokens.dtype))
    gathered = lax.all_gather(own_cols, ("ep", "tp"), axis=0)
    gathered = gathered.reshape(ep, tp, rows, slice_width)

    sig = jax.nn.sigmoid(router_logits)
    gates = 2.827 * sig / jnp.sum(sig, axis=1, keepdims=True)
    named = expert_ids[:, None, :] == jnp.arange(ep, dtype=jnp.int32)[None, :, None]
    dense = jnp.sum(jnp.where(named, gates[:, None, :], 0.0), axis=2)
    dense = jnp.where(live_rows[:, None], dense, 0.0)
    passed = accept_mask * live.astype(jnp.int32)
    count = jnp.sum(jnp.cumprod(passed, axis=1)).astype(jnp.float32)
    sent = jnp.concatenate([dense.T, jnp.broadcast_to(count, (ep, 1))], axis=1)
    got = lax.all_to_all(sent, "ep", split_axis=0, concat_axis=0, tiled=True)
    accepted = jnp.sum(got[:, rows]).astype(jnp.int32).reshape(1)
    gate = got[:, :rows].reshape(ep * rows, 1)

    out = expert(gathered, w_gate, w_up, w_down, gate)
    mixed = lax.psum_scatter(out.reshape(ep * tp, rows, slice_width), ("ep", "tp"), scatter_dimension=0)
    return mixed, accepted


def solution(mesh):
    placed = (
        P(("groups", "ep"), None),
        P("ep", None, "tp"),
        P("ep", None, "tp"),
        P("ep", "tp", None),
        P(("groups", "ep"), None),
        P(("groups", "ep"), None),
        P(("groups", "ep")),
        P(("groups", "ep"), None),
    )
    return jax.shard_map(
        per_device,
        mesh=mesh,
        in_specs=placed,
        out_specs=(P(("groups", "ep"), "tp"), P("groups")),
        check_vma=False,
    )
```

```python
import functools
import jax
import jax.numpy as jnp
from jax import lax
from jax.experimental import pallas as pl
from jax.experimental.pallas import tpu as pltpu
from jax.sharding import Mesh
from jax.sharding import PartitionSpec as P

DRAFT = 8
CORES = 2
EXTRA = 128
CHAINS = 2
F32 = jnp.float32
BF16 = jnp.bfloat16


VMEM = pl.BlockSpec(memory_space=pltpu.VMEM)
SMEM = pl.BlockSpec(memory_space=pltpu.SMEM)


def payload_kernel(ep, lengths, mask, tokens, logits, ids, left):
    rows, half = tokens.shape
    top = ids.shape[1]
    left[:, :half] = tokens[...]
    row = lax.broadcasted_iota(jnp.int32, (rows, EXTRA), 0)
    lane = lax.broadcasted_iota(jnp.int32, (rows, EXTRA), 1)
    count = jnp.int32(0)
    live = jnp.zeros((rows, EXTRA), jnp.int32)
    for r in range(rows // DRAFT):
        prefix = jnp.int32(1)
        for j in range(DRAFT):
            prefix = prefix * mask[r, j] * (j < lengths[r]).astype(jnp.int32)
            count = count + prefix
        live = live + ((row >= r * DRAFT) & (row < r * DRAFT + lengths[r])).astype(jnp.int32)
    sig = 1.0 / (1.0 + jnp.exp(-logits[...]))
    gates = 2.827 * sig / jnp.sum(sig, axis=1, keepdims=True)
    dense = jnp.zeros((rows, EXTRA), F32)
    for k in range(top):
        dense = dense + jnp.where(ids[:, k:k + 1] == lax.rem(lane, ep), gates[:, k:k + 1], 0.0)
    dense = jnp.where(live > 0, dense, 0.0)
    high = dense.astype(BF16).astype(F32)
    extra = jnp.where(lane < ep, high, jnp.where(lane < 2 * ep, dense - high, 0.0))
    extra = jnp.where((lane == 2 * ep) & (row == 0), count.astype(F32), extra)
    left[:, half:] = extra.astype(BF16)


def payload(ep, tokens, logits, ids, lengths, mask):
    rows, half = tokens.shape
    return pl.pallas_call(
        functools.partial(payload_kernel, ep),
        in_specs=[SMEM, SMEM, VMEM, VMEM, VMEM],
        out_specs=VMEM,
        out_shape=jax.ShapeDtypeStruct((rows, half + EXTRA), BF16),
        compiler_params=pltpu.CompilerParams(vmem_limit_bytes=8 << 20),
    )(lengths, mask, tokens, logits, ids)


def ffn_kernel(n, tp, ep, ups, order, place, *refs):
    lefts, rights = refs[:n], refs[n:2 * n]
    weights = refs[2 * n:2 * n + 4]
    wd_own, wd_other = refs[2 * n + 4:2 * n + 6]
    outs, count = refs[2 * n + 6:-4], refs[-4]
    x, acc, hid = refs[-3:]
    step = pl.program_id(0)
    rows = lefts[0].shape[0]
    half = rights[0].shape[1]
    units = weights[0].shape[2]
    block = weights[0].shape[1]

    def spot(i):
        return pl.ds(pl.multiple_of(lax.rem(place[3] + order[i] % n, n) * rows, rows), rows)

    @pl.when(step == 0)
    def _():
        for i in range(n):
            x[spot(i), :half] = lefts[i][:, :half]
            x[spot(i), half:] = rights[i][...]
        acc[...] = jnp.zeros_like(acc)

    @pl.when(step < ups)
    def _():
        piece = x[:, pl.ds(pl.multiple_of(step * block, 128), block)]
        for w in range(4):
            to = slice(w * units, (w + 1) * units)
            acc[:, to] += jnp.dot(piece, weights[w][0], preferred_element_type=F32)

    @pl.when(step == ups - 1)
    def _():
        lane = lax.broadcasted_iota(jnp.int32, (rows, EXTRA), 1)
        total = jnp.zeros((), F32)
        for i in range(n):
            extra = lefts[i][:, half:].astype(F32)
            total = total + jnp.sum(jnp.where(lane == 2 * ep, extra, 0.0))
            for side in range(2):
                e = place[1 + side]
                gate = jnp.sum(jnp.where((lane == e) | (lane == e + ep), extra, 0.0), axis=1, keepdims=True)
                g = acc[spot(i), side * 2 * units:(side * 2 + 1) * units]
                u = acc[spot(i), (side * 2 + 1) * units:(side * 2 + 2) * units]
                hid[spot(i), side * units:(side + 1) * units] = (g / (1.0 + jnp.exp(-g)) * u * gate).astype(BF16)
        count[...] = jnp.full(count.shape, total, F32)

    @pl.when(step >= ups)
    def _():
        out = jnp.dot(hid[:, :units], wd_own[0], preferred_element_type=F32)
        out = out + jnp.dot(hid[:, units:], wd_other[0], preferred_element_type=F32)
        out = out.astype(BF16)
        pos = step - ups
        size = out.shape[0] // CHAINS
        for k in range(tp):
            @pl.when(pos == k)
            def _():
                for c in range(CHAINS):
                    got = out[c * size:(c + 1) * size]
                    if k < tp - 1:
                        outs[c * (tp + 1) + k][...] = got
                    else:
                        outs[c * (tp + 1) + k][...] = got[:size // 2]
                        outs[c * (tp + 1) + k + 1][...] = got[size // 2:]


def ffn(place, order, lefts, rights, weights, downs, tp, ep):
    n, rows = len(lefts), lefts[0].shape[0]
    depth, units = weights[0].shape[1], weights[0].shape[2]
    ups = 4
    width = depth // tp
    total = n * rows
    size = total // CHAINS
    whole = lambda a: pl.BlockSpec(a.shape, lambda s, p: (0, 0))
    up_spec = pl.BlockSpec((1, depth // ups, units), lambda s, p: (0, jnp.minimum(s, ups - 1), 0))

    def column(s, p):
        pos = jnp.maximum(s - ups, 0)
        return (0, 0, lax.rem(p[0] + p[4 + pos], tp))

    down_spec = pl.BlockSpec((1, units, width), column)
    heights = ([size] * (tp - 1) + [size // 2] * 2) * CHAINS
    shapes = [jax.ShapeDtypeStruct((h, width), BF16) for h in heights] + [jax.ShapeDtypeStruct((8, 128), F32)]
    outs = pl.pallas_call(
        functools.partial(ffn_kernel, n, tp, ep, ups, order),
        grid_spec=pltpu.PrefetchScalarGridSpec(
            num_scalar_prefetch=1,
            grid=(ups + tp,),
            in_specs=[whole(a) for a in lefts + rights] + [up_spec] * 4 + [down_spec] * 2,
            out_specs=[pl.BlockSpec(s.shape, lambda s, p: (0, 0)) for s in shapes],
            scratch_shapes=[
                pltpu.VMEM((total, depth), BF16),
                pltpu.VMEM((total, 4 * units), F32),
                pltpu.VMEM((total, 2 * units), BF16),
            ],
        ),
        out_shape=shapes,
        cost_estimate=pl.CostEstimate(
            flops=12 * total * depth * units, bytes_accessed=12 * depth * units, transcendentals=2 * total * units
        ),
        compiler_params=pltpu.CompilerParams(dimension_semantics=("arbitrary",), vmem_limit_bytes=36 << 20),
    )(place, *lefts, *rights, *weights, *downs)
    return [outs[c * (tp + 1):(c + 1) * (tp + 1)] for c in range(CHAINS)], outs[-1]


def added(*terms):
    total = terms[0].astype(F32)
    for t in terms[1:]:
        total = total + t.astype(F32)
    return total.astype(BF16)


def shift(a, axis, s):
    n = lax.axis_size(axis)
    return lax.ppermute(a, axis, [(i, (i + s) % n) for i in range(n)])


def hop(blocks, k, plus, minus):
    a, b = blocks[2 * k - 1], blocks[2 * k]
    h = plus.shape[0]
    if h < a.shape[0]:
        plus = jnp.concatenate([added(a[:h], plus), a[h:]])
        minus = jnp.concatenate([b[:h], added(b[h:], minus)])
    else:
        plus, minus = added(a, plus), added(b, minus)
    return shift(plus, "tp", 1), shift(minus, "tp", -1)


def per_device(tokens, w_gate, w_up, w_down, router_logits, expert_ids, draft_lengths, accept_mask):
    rows, depth = tokens.shape
    ring, tp = lax.axis_size("x"), lax.axis_size("tp")
    ep = ring * CORES
    half = depth // 2
    own, core = lax.axis_index("x"), lax.axis_index("core")
    order = [0, 1, -1, 2, -2, 3, -3, 4]
    place = [lax.axis_index("tp"), CORES * own + core, CORES * own + 1 - core, own] + [k % tp for k in order]
    place = jnp.stack(place).astype(jnp.int32)

    def other(a):
        return shift(a, "core", 1)

    left = payload(ep, tokens[:, :half], router_logits, expert_ids, draft_lengths, accept_mask)
    lefts, rights = {0: left}, {0: tokens[:, half:]}
    for k in range(1, ring // 2):
        rights[-k] = shift(rights[1 - k], "x", 1)
        lefts[-k] = shift(lefts[1 - k], "x", 1)
        rights[k] = shift(rights[k - 1], "x", -1)
        lefts[k] = shift(lefts[k - 1], "x", -1)
    far = ring // 2
    lefts[far] = shift(lefts[1 - far], "x", 1)
    rights[far] = shift(rights[far - 1], "x", -1)

    weights = [w_gate, w_up, other(w_gate), other(w_up)]
    downs = [w_down, other(w_down)]
    chains, count = ffn(place, order, [lefts[k] for k in order], [rights[k] for k in order], weights, downs, tp, ep)
    mine = count[:1, 0].astype(jnp.int32)
    accepted = mine + other(mine)

    state = [(shift(c[7], "tp", 1), shift(c[8], "tp", -1)) for c in chains]
    for k in (3, 2, 1):
        state = [hop(c, k, *s) for c, s in zip(chains, state)]
    summed = jnp.concatenate([added(c[0], *s) for c, s in zip(chains, state)])
    parts = lax.all_to_all(summed.reshape(ring, rows, depth // tp), "x", split_axis=0, concat_axis=0, tiled=True)
    mixed = jnp.sum(parts.astype(F32), axis=0).astype(BF16)
    return mixed, accepted


def solution(mesh):
    groups, ep, tp = (mesh.shape[a] for a in ("groups", "ep", "tp"))
    planes = Mesh(mesh.devices.reshape(groups, ep // CORES, CORES, tp), ("groups", "x", "core", "tp"))
    split = ("x", "core")
    rows = ("groups", *split)
    placed = (
        P(rows, None),
        P(split, None, "tp"),
        P(split, None, "tp"),
        P(split, "tp", None),
        P(rows, None),
        P(rows, None),
        P(rows),
        P(rows, None),
    )
    return jax.shard_map(
        per_device,
        mesh=planes,
        in_specs=placed,
        out_specs=(P(rows, "tp"), P("groups")),
        check_vma=False,
    )
```

```python
import functools
import jax
import jax.numpy as jnp
from jax import lax
from jax.experimental import pallas as pl
from jax.experimental.pallas import tpu as pltpu
from jax.sharding import Mesh
from jax.sharding import PartitionSpec as P

DRAFT = 8
CORES = 2
EXTRA = 128
CHAINS = 2
F32 = jnp.float32
BF16 = jnp.bfloat16


VMEM = pl.BlockSpec(memory_space=pltpu.VMEM)
SMEM = pl.BlockSpec(memory_space=pltpu.SMEM)
HBM = pl.BlockSpec(memory_space=pltpu.HBM)


def payload_kernel(ep, lengths, mask, tokens, logits, ids, left):
    rows, half = tokens.shape
    top = ids.shape[1]
    left[:, :half] = tokens[...]
    row = lax.broadcasted_iota(jnp.int32, (rows, EXTRA), 0)
    lane = lax.broadcasted_iota(jnp.int32, (rows, EXTRA), 1)
    count = jnp.int32(0)
    live = jnp.zeros((rows, EXTRA), jnp.int32)
    for r in range(rows // DRAFT):
        prefix = jnp.int32(1)
        for j in range(DRAFT):
            prefix = prefix * mask[r, j] * (j < lengths[r]).astype(jnp.int32)
            count = count + prefix
        live = live + ((row >= r * DRAFT) & (row < r * DRAFT + lengths[r])).astype(jnp.int32)
    sig = 1.0 / (1.0 + jnp.exp(-logits[...]))
    gates = 2.827 * sig / jnp.sum(sig, axis=1, keepdims=True)
    dense = jnp.zeros((rows, EXTRA), F32)
    for k in range(top):
        dense = dense + jnp.where(ids[:, k:k + 1] == lax.rem(lane, ep), gates[:, k:k + 1], 0.0)
    dense = jnp.where(live > 0, dense, 0.0)
    high = dense.astype(BF16).astype(F32)
    extra = jnp.where(lane < ep, high, jnp.where(lane < 2 * ep, dense - high, 0.0))
    extra = jnp.where((lane == 2 * ep) & (row == 0), count.astype(F32), extra)
    left[:, half:] = extra.astype(BF16)


def payload(ep, tokens, logits, ids, lengths, mask):
    rows, half = tokens.shape
    return pl.pallas_call(
        functools.partial(payload_kernel, ep),
        in_specs=[SMEM, SMEM, VMEM, VMEM, VMEM],
        out_specs=VMEM,
        out_shape=jax.ShapeDtypeStruct((rows, half + EXTRA), BF16),
        compiler_params=pltpu.CompilerParams(vmem_limit_bytes=8 << 20),
    )(lengths, mask, tokens, logits, ids)


def gather_kernel(n, ep, order, place, *refs):
    lefts, rights = refs[:n], refs[n:2 * n]
    x, *gates, count = refs[2 * n:]
    rows = lefts[0].shape[0]
    half = rights[0].shape[1]
    lane = lax.broadcasted_iota(jnp.int32, (rows, EXTRA), 1)
    total = jnp.zeros((), F32)
    for i in range(n):
        at = pl.ds(pl.multiple_of(lax.rem(place[2] + order[i] % n, n) * rows, rows), rows)
        x[at, :half] = lefts[i][:, :half]
        x[at, half:] = rights[i][...]
        extra = lefts[i][:, half:].astype(F32)
        total = total + jnp.sum(jnp.where(lane == 2 * ep, extra, 0.0))
        for side in range(CORES):
            e = place[side]
            gate = jnp.sum(jnp.where((lane == e) | (lane == e + ep), extra, 0.0), axis=1, keepdims=True)
            gates[side][at, :] = jnp.broadcast_to(gate, (rows, gates[side].shape[1]))
    count[...] = jnp.full(count.shape, total, F32)


def gather(place, order, lefts, rights, units, ep):
    n, rows, half = len(rights), *rights[0].shape
    total = n * rows
    shapes = [jax.ShapeDtypeStruct((total, 2 * half), BF16)]
    shapes += [jax.ShapeDtypeStruct((total, units), F32)] * CORES + [jax.ShapeDtypeStruct((8, 128), F32)]
    return pl.pallas_call(
        functools.partial(gather_kernel, n, ep, order),
        in_specs=[SMEM] + [VMEM] * (2 * n),
        out_specs=[VMEM] * len(shapes),
        out_shape=shapes,
        cost_estimate=pl.CostEstimate(flops=total * half, bytes_accessed=8 * total * half, transcendentals=0),
        compiler_params=pltpu.CompilerParams(vmem_limit_bytes=16 << 20),
    )(place, *lefts, *rights)


def preload_kernel(n, *refs):
    sems = refs[2 * n]
    copies = [pltpu.make_async_copy(refs[i], refs[n + i], sems.at[i]) for i in range(n)]
    for c in copies:
        c.start()
    for c in copies:
        c.wait()


def preload(weights):
    n = len(weights)
    size = sum(w.size for w in weights)
    return pl.pallas_call(
        functools.partial(preload_kernel, n),
        in_specs=[HBM] * n,
        out_specs=[VMEM] * n,
        out_shape=[jax.ShapeDtypeStruct(w.shape, w.dtype) for w in weights],
        scratch_shapes=[pltpu.SemaphoreType.DMA((n,))],
        cost_estimate=pl.CostEstimate(flops=size, bytes_accessed=4 * size, transcendentals=0),
        compiler_params=pltpu.CompilerParams(vmem_limit_bytes=14 << 20),
    )(*weights)


def down_kernel(n, order, place, *refs):
    before, gates, ups, weights = (refs[i * n:(i + 1) * n] for i in range(4))
    outs = refs[4 * n:-1]
    hid = refs[-1]
    tp = len(order)
    width = outs[0].shape[1]
    size = outs[0].shape[0]

    for w in range(n):
        g = before[w][...]
        hid[w] = (g / (1.0 + jnp.exp(-g)) * ups[w][...] * gates[w][...]).astype(BF16)
    for k in reversed(range(tp)):
        total = None
        cols = pl.ds(pl.multiple_of(lax.rem(place[0] + order[k] % tp, tp) * width, 128), width)
        for w in range(n):
            term = jnp.dot(hid[w], weights[w][0, :, cols], preferred_element_type=F32)
            total = term if total is None else total + term
        total = total.astype(BF16)
        for c in range(CHAINS):
            got = total[c * size:(c + 1) * size]
            if k < tp - 1:
                outs[c * (tp + 1) + k][...] = got
            else:
                outs[c * (tp + 1) + k][...] = got[:size // 2]
                outs[c * (tp + 1) + k + 1][...] = got[size // 2:]


def down(place, order, before, gates, ups, weights):
    total, units = before[0].shape
    tp = len(order)
    depth = weights[0].shape[2]
    width = depth // tp
    size = total // CHAINS
    heights = ([size] * (tp - 1) + [size // 2] * 2) * CHAINS
    n = len(before)
    outs = pl.pallas_call(
        functools.partial(down_kernel, n, order),
        in_specs=[SMEM] + [VMEM] * (4 * n),
        out_specs=[VMEM] * len(heights),
        out_shape=[jax.ShapeDtypeStruct((h, width), BF16) for h in heights],
        scratch_shapes=[pltpu.VMEM((n, total, units), BF16)],
        cost_estimate=pl.CostEstimate(
            flops=2 * n * total * depth * units, bytes_accessed=2 * n * depth * units, transcendentals=0
        ),
        compiler_params=pltpu.CompilerParams(vmem_limit_bytes=20 << 20),
    )(place, *before, *gates, *ups, *weights)
    return [outs[c * (tp + 1):(c + 1) * (tp + 1)] for c in range(CHAINS)]


def added(*terms):
    total = terms[0].astype(F32)
    for t in terms[1:]:
        total = total + t.astype(F32)
    return total.astype(BF16)


def shift(a, axis, s):
    n = lax.axis_size(axis)
    return lax.ppermute(a, axis, [(i, (i + s) % n) for i in range(n)])


def hop(a, b, plus, minus):
    h = plus.shape[0]
    if h < a.shape[0]:
        plus = jnp.concatenate([added(a[:h], plus), a[h:]])
        minus = jnp.concatenate([b[:h], added(b[h:], minus)])
    else:
        plus, minus = added(a, plus), added(b, minus)
    return shift(plus, "tp", 1), shift(minus, "tp", -1)


def planned(tokens, w_gate, w_up, w_down, router_logits, expert_ids, draft_lengths, accept_mask):
    rows, depth = tokens.shape
    ring, tp = lax.axis_size("x"), lax.axis_size("tp")
    ep = ring * CORES
    half = depth // 2
    own, core = lax.axis_index("x"), lax.axis_index("core")
    order = [0, 1, -1, 2, -2, 3, -3, 4]
    place = jnp.stack([CORES * own + core, CORES * own + 1 - core, own]).astype(jnp.int32)

    def other(a):
        return shift(a, "core", 1)

    opened = shift(tokens[:, half:], "x", 1)
    left = payload(ep, tokens[:, :half], router_logits, expert_ids, draft_lengths, accept_mask)
    lefts, rights = {0: left}, {0: tokens[:, half:]}
    for k in range(1, ring // 2):
        rights[-k] = opened if k == 1 else shift(rights[1 - k], "x", 1)
        lefts[-k] = shift(lefts[1 - k], "x", 1)
        rights[k] = shift(rights[k - 1], "x", -1)
        lefts[k] = shift(lefts[k - 1], "x", -1)
    far = ring // 2
    sides = [(w_gate, w_up, w_down), tuple(other(w) for w in (w_gate, w_up, w_down))]
    lefts[1 - far], rights[far - 1], *theirs = lax.optimization_barrier((lefts[1 - far], rights[far - 1], *sides[1]))
    lefts[far] = shift(lefts[1 - far], "x", 1)
    rights[far] = shift(rights[far - 1], "x", -1)
    sides[1] = preload(theirs)

    x, *gates, count = gather(place, order, [lefts[k] for k in order], [rights[k] for k in order], w_gate.shape[2], ep)
    mine = count[:1, 0].astype(jnp.int32)
    theirs = other(mine)
    accepted = mine + theirs
    before, ups = ([jnp.dot(x, w[i][0], preferred_element_type=F32) for w in sides] for i in range(2))
    chains = down(lax.axis_index("tp").reshape(1), order, before, gates, ups, [w[2] for w in sides])
    width = depth // tp

    state = [(shift(c[7], "tp", 1), shift(c[8], "tp", -1)) for c in chains]
    for k in (3, 2, 1):
        state = [hop(c[2 * k - 1], c[2 * k], *s) for c, s in zip(chains, state)]
    summed = jnp.concatenate([added(c[0], *s) for c, s in zip(chains, state)])
    parts = lax.all_to_all(summed.reshape(ring, rows, width), "x", split_axis=0, concat_axis=0, tiled=True)
    mixed = jnp.sum(parts.astype(F32), axis=0).astype(BF16)
    return mixed, accepted


def solution(mesh):
    groups, ep, tp = (mesh.shape[a] for a in ("groups", "ep", "tp"))
    planes = Mesh(mesh.devices.reshape(groups, ep // CORES, CORES, tp), ("groups", "x", "core", "tp"))
    split = ("x", "core")
    rows = ("groups", *split)
    placed = (
        P(rows, None),
        P(split, None, "tp"),
        P(split, None, "tp"),
        P(split, "tp", None),
        P(rows, None),
        P(rows, None),
        P(rows),
        P(rows, None),
    )
    return jax.shard_map(
        planned,
        mesh=planes,
        in_specs=placed,
        out_specs=(P(rows, "tp"), P("groups")),
        check_vma=False,
    )
```

```python
import functools
import jax
import jax.numpy as jnp
from jax import lax
from jax.experimental import pallas as pl
from jax.experimental.pallas import tpu as pltpu
from jax.sharding import Mesh
from jax.sharding import PartitionSpec as P

DRAFT = 8
CORES = 2
EXTRA = 128
CHAINS = 2
F32 = jnp.float32
BF16 = jnp.bfloat16


VMEM = pl.BlockSpec(memory_space=pltpu.VMEM)
SMEM = pl.BlockSpec(memory_space=pltpu.SMEM)
HBM = pl.BlockSpec(memory_space=pltpu.HBM)


def count_kernel(lengths, mask, total):
    count = jnp.int32(0)
    for r in range(mask.shape[0]):
        prefix = jnp.int32(1)
        for j in range(DRAFT):
            prefix = prefix * mask[r, j] * (j < lengths[r]).astype(jnp.int32)
            count = count + prefix
    total[0] = count


def payload_kernel(ep, lengths, count, tokens, logits, ids, left):
    rows, half = tokens.shape
    top = ids.shape[1]
    left[:, :half] = tokens[...]
    row = lax.broadcasted_iota(jnp.int32, (rows, EXTRA), 0)
    lane = lax.broadcasted_iota(jnp.int32, (rows, EXTRA), 1)
    live = jnp.zeros((rows, EXTRA), jnp.int32)
    for r in range(rows // DRAFT):
        live = live + ((row >= r * DRAFT) & (row < r * DRAFT + lengths[r])).astype(jnp.int32)
    sig = 1.0 / (1.0 + jnp.exp(-logits[...]))
    gates = 2.827 * sig / jnp.sum(sig, axis=1, keepdims=True)
    dense = jnp.zeros((rows, EXTRA), F32)
    for k in range(top):
        dense = dense + jnp.where(ids[:, k:k + 1] == lax.rem(lane, ep), gates[:, k:k + 1], 0.0)
    dense = jnp.where(live > 0, dense, 0.0)
    high = dense.astype(BF16).astype(F32)
    extra = jnp.where(lane < ep, high, jnp.where(lane < 2 * ep, dense - high, 0.0))
    extra = jnp.where((lane == 2 * ep) & (row == 0), count[0].astype(F32), extra)
    left[:, half:] = extra.astype(BF16)


def payload(ep, tokens, logits, ids, lengths, count):
    rows, half = tokens.shape
    return pl.pallas_call(
        functools.partial(payload_kernel, ep),
        in_specs=[SMEM, SMEM, VMEM, VMEM, VMEM],
        out_specs=VMEM,
        out_shape=jax.ShapeDtypeStruct((rows, half + EXTRA), BF16),
        compiler_params=pltpu.CompilerParams(vmem_limit_bytes=8 << 20),
    )(lengths, count, tokens, logits, ids)


def gather_kernel(n, ep, order, place, *refs):
    lefts, rights = refs[:n], refs[n:2 * n]
    x, *gates, count = refs[2 * n:]
    rows = lefts[0].shape[0]
    half = rights[0].shape[1]
    lane = lax.broadcasted_iota(jnp.int32, (rows, EXTRA), 1)
    total = jnp.zeros((), F32)
    for i in range(n):
        at = pl.ds(pl.multiple_of(lax.rem(place[2] + order[i] % n, n) * rows, rows), rows)
        x[at, :half] = lefts[i][:, :half]
        x[at, half:] = rights[i][...]
        extra = lefts[i][:, half:].astype(F32)
        total = total + jnp.sum(jnp.where(lane == 2 * ep, extra, 0.0))
        for side in range(CORES):
            e = place[side]
            gate = jnp.sum(jnp.where((lane == e) | (lane == e + ep), extra, 0.0), axis=1, keepdims=True)
            gates[side][at, :] = jnp.broadcast_to(gate, (rows, gates[side].shape[1]))
    count[...] = jnp.full(count.shape, total, F32)


def gather(place, order, lefts, rights, units, ep):
    n, rows, half = len(rights), *rights[0].shape
    total = n * rows
    shapes = [jax.ShapeDtypeStruct((total, 2 * half), BF16)]
    shapes += [jax.ShapeDtypeStruct((total, units), F32)] * CORES + [jax.ShapeDtypeStruct((8, 128), F32)]
    return pl.pallas_call(
        functools.partial(gather_kernel, n, ep, order),
        in_specs=[SMEM] + [VMEM] * (2 * n),
        out_specs=[VMEM] * len(shapes),
        out_shape=shapes,
        cost_estimate=pl.CostEstimate(flops=total * half, bytes_accessed=8 * total * half, transcendentals=0),
        compiler_params=pltpu.CompilerParams(vmem_limit_bytes=16 << 20),
    )(place, *lefts, *rights)


def preload_kernel(n, *refs):
    sems = refs[2 * n]
    copies = [pltpu.make_async_copy(refs[i], refs[n + i], sems.at[i]) for i in range(n)]
    for c in copies:
        c.start()
    for c in copies:
        c.wait()


def preload(weights):
    n = len(weights)
    size = sum(w.size for w in weights)
    return pl.pallas_call(
        functools.partial(preload_kernel, n),
        in_specs=[HBM] * n,
        out_specs=[VMEM] * n,
        out_shape=[jax.ShapeDtypeStruct(w.shape, w.dtype) for w in weights],
        scratch_shapes=[pltpu.SemaphoreType.DMA((n,))],
        cost_estimate=pl.CostEstimate(flops=size, bytes_accessed=4 * size, transcendentals=0),
        compiler_params=pltpu.CompilerParams(vmem_limit_bytes=14 << 20),
    )(*weights)


def down_kernel(n, order, place, *refs):
    before, gates, ups, weights = (refs[i * n:(i + 1) * n] for i in range(4))
    outs = refs[4 * n:-1]
    hid = refs[-1]
    tp = len(order)
    width = outs[0].shape[1]
    size = outs[0].shape[0]

    for w in range(n):
        g = before[w][...]
        hid[w] = (g / (1.0 + jnp.exp(-g)) * ups[w][...] * gates[w][...]).astype(BF16)
    for k in reversed(range(tp)):
        total = None
        cols = pl.ds(pl.multiple_of(lax.rem(place[0] + order[k] % tp, tp) * width, 128), width)
        for w in range(n):
            term = jnp.dot(hid[w], weights[w][0, :, cols], preferred_element_type=F32)
            total = term if total is None else total + term
        total = total.astype(BF16)
        for c in range(CHAINS):
            got = total[c * size:(c + 1) * size]
            if k < tp - 1:
                outs[c * (tp + 1) + k][...] = got
            else:
                outs[c * (tp + 1) + k][...] = got[:size // 2]
                outs[c * (tp + 1) + k + 1][...] = got[size // 2:]


def down(place, order, before, gates, ups, weights):
    total, units = before[0].shape
    tp = len(order)
    depth = weights[0].shape[2]
    width = depth // tp
    size = total // CHAINS
    heights = ([size] * (tp - 1) + [size // 2] * 2) * CHAINS
    n = len(before)
    outs = pl.pallas_call(
        functools.partial(down_kernel, n, order),
        in_specs=[SMEM] + [VMEM] * (4 * n),
        out_specs=[VMEM] * len(heights),
        out_shape=[jax.ShapeDtypeStruct((h, width), BF16) for h in heights],
        scratch_shapes=[pltpu.VMEM((n, total, units), BF16)],
        cost_estimate=pl.CostEstimate(
            flops=2 * n * total * depth * units, bytes_accessed=2 * n * depth * units, transcendentals=0
        ),
        compiler_params=pltpu.CompilerParams(vmem_limit_bytes=20 << 20),
    )(place, *before, *gates, *ups, *weights)
    return [outs[c * (tp + 1):(c + 1) * (tp + 1)] for c in range(CHAINS)]


def added(*terms):
    total = terms[0].astype(F32)
    for t in terms[1:]:
        total = total + t.astype(F32)
    return total.astype(BF16)


def shift(a, axis, s):
    n = lax.axis_size(axis)
    return lax.ppermute(a, axis, [(i, (i + s) % n) for i in range(n)])


def hop(a, b, plus, minus):
    h = plus.shape[0]
    if h < a.shape[0]:
        plus = jnp.concatenate([added(a[:h], plus), a[h:]])
        minus = jnp.concatenate([b[:h], added(b[h:], minus)])
    else:
        plus, minus = added(a, plus), added(b, minus)
    return shift(plus, "tp", 1), shift(minus, "tp", -1)


def planned(tokens, w_gate, w_up, w_down, router_logits, expert_ids, draft_lengths, accept_mask):
    rows, depth = tokens.shape
    ring, tp = lax.axis_size("x"), lax.axis_size("tp")
    ep = ring * CORES
    half = depth // 2
    own, core = lax.axis_index("x"), lax.axis_index("core")
    order = [0, 1, -1, 2, -2, 3, -3, 4]
    place = jnp.stack([CORES * own + core, CORES * own + 1 - core, own]).astype(jnp.int32)

    def other(a):
        return shift(a, "core", 1)

    mine = pl.pallas_call(
        count_kernel, in_specs=[SMEM, SMEM], out_specs=SMEM, out_shape=jax.ShapeDtypeStruct((1,), jnp.int32)
    )(draft_lengths, accept_mask)
    theirs = other(mine)
    sides = [(w_gate, w_up, w_down), tuple(other(w) for w in (w_gate, w_up, w_down))]
    opened = shift(tokens[:, half:], "x", 1)
    mirrored = shift(tokens[:, half:], "x", -1)
    left = payload(ep, tokens[:, :half], router_logits, expert_ids, draft_lengths, mine + theirs)
    lefts, rights = {0: left}, {0: tokens[:, half:]}
    for k in range(1, ring // 2):
        rights[-k] = opened if k == 1 else shift(rights[1 - k], "x", 1)
        lefts[-k] = shift(lefts[1 - k], "x", 1)
        rights[k] = mirrored if k == 1 else shift(rights[k - 1], "x", -1)
        lefts[k] = shift(lefts[k - 1], "x", -1)
    far = ring // 2
    lefts[1 - far], rights[far - 1], *theirs = lax.optimization_barrier((lefts[1 - far], rights[far - 1], *sides[1]))
    lefts[far] = shift(lefts[1 - far], "x", 1)
    rights[far] = shift(rights[far - 1], "x", -1)
    sides[1] = preload(sides[1])

    x, *gates, count = gather(place, order, [lefts[k] for k in order], [rights[k] for k in order], w_gate.shape[2], ep)
    accepted = count[:1, 0].astype(jnp.int32)
    before, ups = ([jnp.dot(x, w[i][0], preferred_element_type=F32) for w in sides] for i in range(2))
    chains = down(lax.axis_index("tp").reshape(1), order, before, gates, ups, [w[2] for w in sides])
    width = depth // tp

    state = [(shift(c[7], "tp", 1), shift(c[8], "tp", -1)) for c in chains]
    state = [hop(c[5], c[6], *s) for c, s in zip(chains, state)]
    for k in (2, 1):
        state = [hop(c[2 * k - 1], c[2 * k], *s) for c, s in zip(chains, state)]
    summed = jnp.concatenate([added(c[0], *s) for c, s in zip(chains, state)])
    parts = lax.all_to_all(summed.reshape(ring, rows, width), "x", split_axis=0, concat_axis=0, tiled=True)
    mixed = jnp.sum(parts.astype(F32), axis=0).astype(BF16)
    return mixed, accepted


def solution(mesh):
    groups, ep, tp = (mesh.shape[a] for a in ("groups", "ep", "tp"))
    planes = Mesh(mesh.devices.reshape(groups, ep // CORES, CORES, tp), ("groups", "x", "core", "tp"))
    split = ("x", "core")
    rows = ("groups", *split)
    placed = (
        P(rows, None),
        P(split, None, "tp"),
        P(split, None, "tp"),
        P(split, "tp", None),
        P(rows, None),
        P(rows, None),
        P(rows),
        P(rows, None),
    )
    return jax.shard_map(
        planned,
        mesh=planes,
        in_specs=placed,
        out_specs=(P(rows, "tp"), P("groups")),
        check_vma=False,
    )
```
